32 devices in a mesh: row: 4 (over z), col: 8 (over y, x, core).
Axes of the slice: x: 2, y: 2, z: 4, core: 2. Of those that a mesh axis runs over, the one named last changes fastest.
Arguments:
- clean: float32 [1344, 8192], P('row', 'col'), may hold values from -6 to 6
- noise: float32 [1344, 8192], P('row', 'col'), may hold values from -6 to 6
- bucket: int32 [32], replicated, may hold values from 0 to 31
- mod_table: float32 [1, 32, 1344], replicated, may hold values from -3 to 3
- w_first: float32 [1, 1344, 1344], P(None, 'row', 'col'), may hold values from -0.15625 to 0.15625
- w_second: float32 [1, 1344, 1344], P(None, 'col', 'row'), may hold values from -0.15625 to 0.15625
Outputs:
- grad_first: float32 [1, 1344, 1344], P(None, 'row', 'col')
- grad_second: float32 [1, 1344, 1344], P(None, 'col', 'row')
The draws below stay inside these ranges and needn't reach their ends.
All inputs are finite; a program needn't handle non-finite values.
Results may differ from the reference program's by a relative error of at most 0.018.
Values may be sent and summed in bfloat16 or wider, within the bound.
A program may use at most 64 MiB of HBM per device.

```python
import math
import jax
import jax.numpy as jnp
from jax import lax

WIDTH = 1344
PIX = 256
BLOCKS = 1
BUCKETS = 32
SAMPLES = 32


def place_ends(array, own_key, least, top_value):
    longest = array.shape.index(max(array.shape))
    spots = []
    for shift in (0, 1):
        where = [jax.random.randint(jax.random.fold_in(own_key, axis), (), 0, length) for axis, length in enumerate(array.shape)]
        where[longest] = (where[longest] + shift) % array.shape[longest]
        spots.append(tuple(where))
    return array.at[spots[0]].set(least).at[spots[1]].set(top_value)


def shard_levels(rng, extent, cuts, low, high):
    def one(dim, shards_of):
        heights = jax.random.uniform(jax.random.fold_in(jax.random.fold_in(rng, 6), dim), (shards_of,), jnp.float32, low / len(cuts), high / len(cuts))
        return jnp.repeat(jnp.exp(heights), extent[dim] // shards_of).reshape((-1,) + (1,) * (len(extent) - dim - 1))

    level = one(*cuts[0])
    for cut in cuts[1:]:
        level = level * one(*cut)
    return level


def scatter_about(stream_key, dims, deviation, bound, cuts=(), kind=jnp.bfloat16):
    values = jax.random.normal(stream_key, dims, jnp.float32) * deviation
    if len(cuts) > 0:
        values = shard_levels(stream_key, dims, cuts, -0.22, 0.18) * values
    return jnp.clip(values, min=-bound, max=bound).astype(kind)


def setup_inputs(seed: int = 0) -> dict:
    seeds = jax.random.split(jax.random.key(seed), 7)
    clean = scatter_about(seeds[0], (WIDTH, SAMPLES * PIX), 1.0, 6.0, ((0, 4), (1, 8)), jnp.float32)
    noise = scatter_about(seeds[1], (WIDTH, SAMPLES * PIX), 1.0, 6.0, ((0, 4), (1, 8)), jnp.float32)
    bucket = place_ends(jax.random.randint(seeds[2], (SAMPLES,), 0, BUCKETS), jax.random.fold_in(seeds[2], 1), 0, BUCKETS - 1).astype(jnp.int32)
    mod_table = scatter_about(seeds[3], (BLOCKS, BUCKETS, WIDTH), 0.3, 3.0, (), jnp.float32)
    w_first = scatter_about(seeds[4], (BLOCKS, WIDTH, WIDTH), WIDTH ** -0.5, 0.15625, ((1, 4), (2, 8)), jnp.float32)
    w_second = scatter_about(seeds[5], (BLOCKS, WIDTH, WIDTH), WIDTH ** -0.5, 0.15625, ((1, 8), (2, 4)), jnp.float32)
    return dict(clean=clean, noise=noise, bucket=bucket, mod_table=mod_table, w_first=w_first, w_second=w_second)


MIX_WEIGHT = 0.3
KEEP_COEF = (1.0 - MIX_WEIGHT) / math.sqrt((1.0 - MIX_WEIGHT) ** 2 + MIX_WEIGHT ** 2)
ADD_COEF = MIX_WEIGHT / math.sqrt((1.0 - MIX_WEIGHT) ** 2 + MIX_WEIGHT ** 2)
SILU_GAIN = 1.0 / 0.596

def noise_levels(bucket):
    return jnp.exp(-3.0 + 5.0 * (bucket.astype(jnp.float32) + 0.5) / BUCKETS)

def silu_slope(values):
    sig = jax.nn.sigmoid(values)
    return sig * (1.0 + values * (1.0 - sig))

def reference(clean, noise, bucket, mod_table, w_first, w_second):
    clean = clean.T
    noise = noise.T
    levels = jnp.repeat(noise_levels(bucket), PIX)[:, None]
    spread_root = jnp.sqrt(levels * levels + 0.25)
    state = ((clean + levels * noise) / spread_root).astype(jnp.bfloat16)
    target = clean * (2.0 * levels / spread_root) - noise * (0.5 / spread_root)
    onehot = (bucket[:, None] == jnp.arange(BUCKETS, dtype=jnp.int32)[None, :]).astype(jnp.float32)
    saved = []
    for block in range(BLOCKS):
        col_first = jnp.sqrt(lax.optimization_barrier(jnp.sum(w_first[block] * w_first[block], axis=0)) + 1.0)
        col_second = jnp.sqrt(lax.optimization_barrier(jnp.sum(w_second[block] * w_second[block], axis=0)) + 1.0)
        normed_first = (w_first[block] / col_first[None, :]).astype(jnp.bfloat16)
        normed_second = (w_second[block] / col_second[None, :]).astype(jnp.bfloat16)
        gains = jnp.dot(onehot, 1.0 + mod_table[block], precision=lax.Precision.HIGHEST, preferred_element_type=jnp.float32)
        gains = jnp.repeat(gains, PIX, axis=0)
        pre_act = jnp.dot(state, normed_first, preferred_element_type=jnp.float32)
        hidden = (jax.nn.silu(pre_act) * SILU_GAIN * gains).astype(jnp.bfloat16)
        branch = jnp.dot(hidden, normed_second, preferred_element_type=jnp.float32)
        saved.append((state, hidden, pre_act, gains, normed_first, normed_second, col_first, col_second))
        state = (KEEP_COEF * state.astype(jnp.float32) + ADD_COEF * branch).astype(jnp.bfloat16)
    grad_state = (state.astype(jnp.float32) - target) / SAMPLES
    firsts = []
    seconds = []
    for block in range(BLOCKS - 1, -1, -1):
        state_in, hidden, pre_act, gains, normed_first, normed_second, col_first, col_second = saved[block]
        dbranch = (ADD_COEF * grad_state).astype(jnp.bfloat16)
        gsecond = jnp.dot(hidden.T, dbranch, preferred_element_type=jnp.float32)
        dhidden = jnp.dot(dbranch, normed_second.T, preferred_element_type=jnp.float32)
        dpre = (dhidden * gains * silu_slope(pre_act) * SILU_GAIN).astype(jnp.bfloat16)
        gfirst = jnp.dot(state_in.T, dpre, preferred_element_type=jnp.float32)
        if block > 0:
            grad_state = KEEP_COEF * grad_state + jnp.dot(dpre, normed_first.T, preferred_element_type=jnp.float32)
        dot_first = lax.optimization_barrier(jnp.sum(w_first[block] * gfirst, axis=0))
        dot_second = lax.optimization_barrier(jnp.sum(w_second[block] * gsecond, axis=0))
        firsts.append(gfirst / col_first[None, :] - w_first[block] * (dot_first / col_first ** 3)[None, :])
        seconds.append(gsecond / col_second[None, :] - w_second[block] * (dot_second / col_second ** 3)[None, :])
    grad_first = jnp.stack(firsts[::-1], axis=0)
    grad_second = jnp.stack(seconds[::-1], axis=0)
    return (grad_first, grad_second)
```

```python
import math

import jax
import jax.numpy as jnp
from jax import lax
from jax.experimental import pallas as pl
from jax.experimental.pallas import tpu as pltpu
from jax.sharding import PartitionSpec as P

PIX = 256
BUCKETS = 32


MIX_WEIGHT = 0.3
KEEP_COEF = (1.0 - MIX_WEIGHT) / math.sqrt((1.0 - MIX_WEIGHT) ** 2 + MIX_WEIGHT**2)
ADD_COEF = MIX_WEIGHT / math.sqrt((1.0 - MIX_WEIGHT) ** 2 + MIX_WEIGHT**2)
SILU_GAIN = 1.0 / 0.596
CONTRACT_LEAD = (((0,), (0,)), ((), ()))
CONTRACT_TAIL = (((1,), (1,)), ((), ()))


def noise_levels(bucket):
    return jnp.exp(-3.0 + 5.0 * (bucket.astype(jnp.float32) + 0.5) / BUCKETS)


def silu_slope(values):
    sig = jax.nn.sigmoid(values)
    return sig * (1.0 + values * (1.0 - sig))


def bucket_gains(table, picked):
    onehot = (picked[:, None] == jnp.arange(table.shape[0], dtype=jnp.int32)[None, :]).astype(
        jnp.float32
    )
    return jnp.dot(
        onehot, table, precision=lax.Precision.HIGHEST, preferred_element_type=jnp.float32
    )


def local(clean, noise, bucket, mod_table, w_first, w_second):
    rows_size = lax.axis_size("row")
    row_at = lax.axis_index("row")
    col_at = lax.axis_index("col")
    samples = bucket.shape[0]
    own_rows = clean.shape[1]
    weight_first = w_first[0]
    weight_second = w_second[0]
    table = 1.0 + mod_table[0]
    col_first = jnp.sqrt(lax.psum(jnp.sum(weight_first * weight_first, axis=0), "row") + 1.0)
    col_second = jnp.sqrt(lax.psum(jnp.sum(weight_second * weight_second, axis=0), "col") + 1.0)
    normed_first = (weight_first / col_first[None, :]).astype(jnp.bfloat16)
    normed_second = (weight_second / col_second[None, :]).astype(jnp.bfloat16)
    chan_clean, chan_noise = (
        lax.all_to_all(
            clean.astype(jnp.bfloat16), "row", split_axis=1, concat_axis=0, tiled=True
        ).astype(clean.dtype),
        lax.all_to_all(
            noise.astype(jnp.bfloat16), "row", split_axis=1, concat_axis=0, tiled=True
        ).astype(noise.dtype),
    )
    local_clean = chan_clean.T
    local_noise = chan_noise.T
    sub_rows = own_rows // rows_size
    first_row = col_at * own_rows + row_at * sub_rows
    row_sample = (first_row + jnp.arange(sub_rows, dtype=jnp.int32)) // PIX
    row_bucket = jnp.take(bucket, row_sample)
    levels = noise_levels(row_bucket)[:, None]
    spread_root = jnp.sqrt(levels * levels + 0.25)
    state_own = ((local_clean + levels * local_noise) / spread_root).astype(jnp.bfloat16)
    target = local_clean * (2.0 * levels / spread_root) - local_noise * (0.5 / spread_root)
    gains = bucket_gains(table, row_bucket)
    part_first, part_second = (
        lax.all_gather(normed_first, "col", axis=1, tiled=True),
        lax.all_gather(normed_second, "col", axis=0, tiled=True),
    )
    full_first, full_second = (
        lax.all_gather(part_first, "row", axis=0, tiled=True),
        lax.all_gather(part_second, "row", axis=1, tiled=True),
    )
    pre_act = jnp.dot(state_own, full_first, preferred_element_type=jnp.float32)
    hidden = (jax.nn.silu(pre_act) * SILU_GAIN * gains).astype(jnp.bfloat16)
    branch = jnp.dot(hidden, full_second, preferred_element_type=jnp.float32)
    state_new = (KEEP_COEF * state_own.astype(jnp.float32) + ADD_COEF * branch).astype(jnp.bfloat16)
    grad_own = (state_new.astype(jnp.float32) - target) / samples
    dbranch = (ADD_COEF * grad_own).astype(jnp.bfloat16)
    gsecond_full = lax.dot_general(
        hidden, dbranch, CONTRACT_LEAD, preferred_element_type=jnp.float32
    )
    dhidden = lax.dot_general(
        dbranch, full_second, CONTRACT_TAIL, preferred_element_type=jnp.float32
    )
    dpre = (dhidden * gains * silu_slope(pre_act) * SILU_GAIN).astype(jnp.bfloat16)
    gfirst_full = lax.dot_general(
        state_own, dpre, CONTRACT_LEAD, preferred_element_type=jnp.float32
    )
    part_gfirst, part_gsecond = (
        lax.psum_scatter(
            gfirst_full.astype(jnp.bfloat16), "col", scatter_dimension=1, tiled=True
        ).astype(jnp.float32),
        lax.psum_scatter(
            gsecond_full.astype(jnp.bfloat16), "col", scatter_dimension=0, tiled=True
        ).astype(jnp.float32),
    )
    gfirst, gsecond = (
        lax.psum_scatter(
            part_gfirst.astype(jnp.bfloat16), "row", scatter_dimension=0, tiled=True
        ).astype(jnp.float32),
        lax.psum_scatter(
            part_gsecond.astype(jnp.bfloat16), "row", scatter_dimension=1, tiled=True
        ).astype(jnp.float32),
    )
    dot_first = lax.psum(jnp.sum(weight_first * gfirst, axis=0), "row")
    dot_second = lax.psum(jnp.sum(weight_second * gsecond, axis=0), "col")
    grad_first = gfirst / col_first[None, :] - weight_first * (dot_first / col_first**3)[None, :]
    grad_second = (
        gsecond / col_second[None, :] - weight_second * (dot_second / col_second**3)[None, :]
    )
    return (grad_first[None], grad_second[None])


CORES = 2
SIDE = 2
MESH = pl.DeviceIdType.MESH
(S_UP, S_DN, S_X, S_Y, S_D0, S_D1, S_S, S_T, S_F, R_Z, R_X, R_Y, R_D0, R_D1, R_S, R_T, R_F,
 S_A0, S_A1, R_A0, R_A1, S_BX, S_CX, S_BY, S_CY, R_BX, R_CX, R_BY, R_CY, S_P, R_P, MISC) = range(32)


def round_up(size, unit):
    return -(-size // unit) * unit


def step_kernel(
    hb, ib, samples, wown, sto, gsel, w1f, w2f, out1, out2,
    w, st, tg, pre, hid, brp, brk, brr, dbr, db2, dpre, s2, d2, g,
    ra, sa, rx, ry, pz, rz, colf, sems,
):
    rows = st.shape[1] // wown.shape[2]
    hp, ip = wown.shape[1], wown.shape[2]
    chips = w.shape[1] // hp
    sub = st.shape[2]
    z = lax.axis_index("row")
    col = lax.axis_index("col")
    core = lax.rem(col, CORES)
    xy = col // CORES
    x, y = lax.rem(xy, SIDE), xy // SIDE
    xn = y * SIDE + (1 - x)
    yn = (1 - y) * SIDE + x
    dn = (1 - y) * SIDE + (1 - x)
    dev_x = (z, xn * CORES + core)
    dev_y = (z, yn * CORES + core)
    dev_p = (z, xy * CORES + 1 - core)
    up, down = (z + 1, col), (z - 1, col)
    ring = [lax.rem(z + k, rows) for k in range(rows)]

    barrier = pltpu.get_barrier_semaphore()
    peers = [dev_x, dev_y, dev_p] + [(ring[k], col) for k in range(1, rows)]
    for peer in peers:
        pl.semaphore_signal(barrier, inc=1, device_id=peer, device_id_type=MESH)

    pending = []

    def remote(src, dst, send, recv, dev):
        return pltpu.make_async_remote_copy(
            src_ref=src, dst_ref=dst, send_sem=sems.at[send[0], send[1]],
            recv_sem=sems.at[recv[0], recv[1]], device_id=dev, device_id_type=MESH,
        )

    def when(cond, fn):
        if cond is None:
            fn()
        else:
            pl.when(cond)(fn)

    def send(cond, *spec):
        when(cond, lambda: remote(*spec).start())
        pending.append((cond, spec))

    def arrive(cond, dst, recv):
        when(cond, lambda: remote(dst, dst, recv, recv, dev_p).wait_recv())

    def both(a, b):
        return b if a is None else (a if b is None else jnp.logical_and(a, b))

    def blk(zb, xyb, half=None):
        at = (pl.ds(pl.multiple_of(xyb * hp, 16), hp), pl.ds(pl.multiple_of(zb * ip, 128), ip))
        return w.at[(slice(None),) + at] if half is None else w.at[(half,) + at]

    def chan(zb):
        return pl.ds(pl.multiple_of(zb * ip, 128), ib)

    def pix(zb):
        return pl.ds(pl.multiple_of(zb * sub, 128), sub)

    local_w = pltpu.make_async_copy(wown, blk(z, xy), sems.at[MISC, 0])
    local_w.start()
    local_s = pltpu.make_async_copy(sto.at[0, :, pix(z)], st.at[core, chan(z)], sems.at[MISC, 1])
    local_s.start()
    local_t = pltpu.make_async_copy(sto.at[1, :, pix(z)], tg.at[chan(z)], sems.at[MISC, 2])
    local_t.start()
    for zb in range(rows):
        pad = slice(zb * ip + ib, (zb + 1) * ip)
        zero = jnp.zeros((ip - ib, sub), jnp.bfloat16)
        st[0, pad, :] = zero
        st[1, pad, :] = zero
        tg[pad, :] = zero
    pl.semaphore_wait(barrier, len(peers))

    def spread(cond, zb, src, go_up, go_down):
        if go_up:
            send(both(cond, z + 1 < rows), src, blk(zb, xy), (S_UP, zb), (R_Z, zb), up)
        if go_down:
            send(both(cond, z > 0), src, blk(zb, xy), (S_DN, zb), (R_Z, zb), down)
        send(cond, src, blk(zb, xy), (S_X, zb), (R_X, zb), dev_x)
        send(cond, src, blk(zb, xy), (S_Y, zb), (R_Y, zb), dev_y)

    def state_out(k):
        zt = ring[k]
        send(None, sto.at[0, :, pix(zt)], st.at[core, chan(z)], (S_S, k), (R_S, z), (zt, col))

    def diagonal(cond, zb):
        arrive(cond, blk(zb, xn), (R_X, zb))
        send(cond, blk(zb, xn, 0), blk(zb, xn, 0), (S_D0, zb), (R_D0, zb), dev_y)
        arrive(cond, blk(zb, yn), (R_Y, zb))
        send(cond, blk(zb, yn, 1), blk(zb, yn, 1), (S_D1, zb), (R_D1, zb), dev_x)

    spread(None, z, wown, True, True)
    send(None, sto.at[0, :, pix(z)], st.at[core, chan(z)], (S_F, z), (R_F, z), dev_p)
    for d in range(1, rows + 1):
        if d < rows:
            state_out(d)
            low, high = z - d, z + d
            arrive(low >= 0, blk(low, xy), (R_Z, low))
            spread(low >= 0, low, blk(low, xy), True, False)
            arrive(high < rows, blk(high, xy), (R_Z, high))
            spread(high < rows, high, blk(high, xy), False, True)
        if d == 1:
            diagonal(None, z)
        else:
            diagonal(z - (d - 1) >= 0, z - (d - 1))
            diagonal(z + (d - 1) < rows, z + (d - 1))
        if d == rows - 1:
            for k in range(1, rows):
                zt = ring[k]
                send(None, sto.at[1, :, pix(zt)], tg.at[chan(z)], (S_T, k), (R_T, z), (zt, col))
    for k in range(1, rows):
        zb = ring[rows - k]
        arrive(None, st.at[core, chan(zb)], (R_S, zb))
        send(None, st.at[core, chan(zb)], st.at[core, chan(zb)], (S_F, zb), (R_F, zb), dev_p)
    for zb in range(rows):
        arrive(None, blk(zb, dn, 0), (R_D0, zb))
        arrive(None, blk(zb, dn, 1), (R_D1, zb))
    local_w.wait()
    local_s.wait()
    local_t.wait()

    half_rows = w.shape[1] // 2
    for part in range(2):
        at = slice(part * half_rows, (part + 1) * half_rows)
        block = w[0, at, :].astype(jnp.float32)
        colf[at, :] = jnp.broadcast_to(
            jnp.sqrt(1.0 + jnp.sum(block * block, axis=1, keepdims=True)), (half_rows, colf.shape[1])
        )
    total = jnp.zeros((1, w.shape[2]), jnp.float32)
    for part in range(2):
        block = w[1, part * half_rows : (part + 1) * half_rows, :].astype(jnp.float32)
        total = total + jnp.sum(block * block, axis=0, keepdims=True)
    s2[0] = jnp.broadcast_to(total, s2.shape[1:])
    send(None, s2.at[0], s2.at[1], (MISC, 3), (MISC, 4), dev_p)
    for zb in range(rows):
        arrive(None, st.at[1 - core, chan(zb)], (R_F, zb))

    def forward(j):
        @pl.loop(0, 2)
        def _(part):
            at = pl.ds(pl.multiple_of(part * half_rows, 16), half_rows)
            value = jnp.dot(w[0, at, :], st[j], preferred_element_type=jnp.float32)
            value = value / colf[at, :1]
            pre[j, at, :] = value
            hid[j, at, :] = (value * jax.nn.sigmoid(value) * SILU_GAIN * gsel[j, at, :]).astype(jnp.bfloat16)

    def branch_part(j, dst):
        @pl.loop(0, rows)
        def _(zb):
            at = pl.ds(pl.multiple_of(zb * ip, 128), ip)
            dst[at, :] = lax.dot_general(
                w[1, :, at], hid[j], CONTRACT_LEAD, preferred_element_type=jnp.float32
            )

    forward(1 - core)
    branch_part(1 - core, brp)
    send(None, brp, brr, (MISC, 5), (MISC, 6), dev_p)
    forward(core)
    branch_part(core, brk)
    for k in range(1, rows):
        arrive(None, tg.at[chan(ring[k])], (R_T, ring[k]))
    arrive(None, s2.at[1], (MISC, 4))
    col2_row = jnp.sqrt(1.0 + s2[0] + s2[1])
    col2 = col2_row.T[:, :1]
    arrive(None, brr, (MISC, 6))
    for zb in range(rows):
        at = slice(zb * ip, (zb + 1) * ip)
        norm = col2[at, :]
        branch = (brk[at, :] + brr[at, :]) / norm
        fresh = (KEEP_COEF * st[core, at, :].astype(jnp.float32) + ADD_COEF * branch).astype(jnp.bfloat16)
        slope = (fresh.astype(jnp.float32) - tg[at, :].astype(jnp.float32)) / samples
        rounded = (ADD_COEF * slope).astype(jnp.bfloat16)
        dbr[core, at, :] = rounded
        product = jnp.sum(branch * rounded.astype(jnp.float32), axis=1, keepdims=True) * norm
        d2[0, :, at] = jnp.broadcast_to(product, (ip, 128)).T[: d2.shape[1], :]
    send(None, dbr.at[core], dbr.at[core], (MISC, 7), (MISC, 8), dev_p)
    send(None, d2.at[0], d2.at[1], (MISC, 9), (MISC, 10), dev_p)

    def scale_back(j):
        for zb in range(rows):
            at = slice(zb * ip, (zb + 1) * ip)
            db2[j, at, :] = (dbr[j, at, :].astype(jnp.float32) / col2[at, :]).astype(jnp.bfloat16)

    def backward(j):
        @pl.loop(0, 2)
        def _(part):
            at = pl.ds(pl.multiple_of(part * half_rows, 16), half_rows)
            grad = jnp.dot(w[1, at, :], db2[j], preferred_element_type=jnp.float32)
            dpre[j, at, :] = (grad * gsel[j, at, :] * silu_slope(pre[j, at, :]) * SILU_GAIN).astype(jnp.bfloat16)

    scale_back(core)
    backward(core)
    arrive(None, dbr.at[1 - core], (MISC, 8))
    arrive(None, d2.at[1], (MISC, 10))
    scale_back(1 - core)
    backward(1 - core)
    dot1 = colf[:, :1] * sum(
        jnp.sum(dpre[j].astype(jnp.float32) * pre[j], axis=1, keepdims=True) for j in range(CORES)
    )
    lane = lax.broadcasted_iota(jnp.int32, (1, ip), 1)
    line = lax.broadcasted_iota(jnp.int32, (hp, 1), 0)

    def gradients(zb):
        at = pl.ds(pl.multiple_of(zb * ip, 128), ip)
        first = sum(
            lax.dot_general(dpre[j], st[j, at, :], CONTRACT_TAIL, preferred_element_type=jnp.float32)
            for j in range(CORES)
        )
        g[0, :, at] = jnp.where(lane >= ib, dot1, first).astype(jnp.bfloat16)
        second = sum(
            lax.dot_general(hid[j], dbr[j, at, :], CONTRACT_TAIL, preferred_element_type=jnp.float32)
            for j in range(CORES)
        )
        dot2 = d2[0, :1, at] + d2[1, :1, at]
        for b in range(chips):
            part = second[b * hp : (b + 1) * hp, :]
            g[1, b * hp : (b + 1) * hp, at] = jnp.where(line >= hb, dot2, part).astype(jnp.bfloat16)

    def gblk(half, xyb, zb):
        return (half, pl.ds(pl.multiple_of(xyb * hp, 16), hp), pl.ds(pl.multiple_of(zb * ip, 128), ip))

    order = ring[1:] + ring[:1]

    def stage_a(k):
        zb = order[k]
        send(None, g.at[gblk(0, dn, zb)], ra.at[0, k], (S_A0, k), (R_A0, k), dev_y)
        send(None, g.at[gblk(1, dn, zb)], ra.at[1, k], (S_A1, k), (R_A1, k), dev_x)
        send(None, g.at[gblk(1, xn, zb)], rx.at[1, k], (S_CX, k), (R_CX, k), dev_x)
        send(None, g.at[gblk(0, yn, zb)], ry.at[0, k], (S_CY, k), (R_CY, k), dev_y)

    def wide(value):
        return value.astype(jnp.float32)

    def stage_b(k):
        zb = order[k]
        arrive(None, ra.at[0, k], (R_A0, k))
        sa[0, k] = (wide(g[gblk(0, xn, zb)]) + wide(ra[0, k])).astype(jnp.bfloat16)
        send(None, sa.at[0, k], rx.at[0, k], (S_BX, k), (R_BX, k), dev_x)
        arrive(None, ra.at[1, k], (R_A1, k))
        sa[1, k] = (wide(g[gblk(1, yn, zb)]) + wide(ra[1, k])).astype(jnp.bfloat16)
        send(None, sa.at[1, k], ry.at[1, k], (S_BY, k), (R_BY, k), dev_y)

    def stage_c(k):
        zb = order[k]
        arrive(None, rx.at[1, k], (R_CX, k))
        arrive(None, ry.at[0, k], (R_CY, k))
        arrive(None, rx.at[0, k], (R_BX, k))
        arrive(None, ry.at[1, k], (R_BY, k))
        sums = [wide(g[gblk(half, xy, zb)]) + wide(rx[half, k]) + wide(ry[half, k]) for half in range(2)]
        if k == rows - 1:
            return sums
        pz[k, 0] = sums[0].astype(jnp.bfloat16)
        pz[k, 1] = sums[1].astype(jnp.bfloat16)
        send(None, pz.at[k], rz.at[k], (S_P, k), (R_P, k), (zb, col))
        return None

    for k in range(rows):
        gradients(order[k])
        stage_a(k)
        if k >= 1:
            stage_b(k - 1)
    sums = None
    for k in range(rows):
        if k == rows - 2:
            stage_b(rows - 1)
        sums = stage_c(k)
    for k in range(rows - 1):
        arrive(None, rz.at[k], (R_P, k))
    first, second = (
        sums[half] + sum(wide(rz[k, half]) for k in range(rows - 1)) for half in range(2)
    )
    norm1 = colf[pl.ds(pl.multiple_of(xy * hp, 16), hp), :1][:hb]
    dot_first = first[:hb, ib : ib + 1]
    out1[...] = first[:hb, :ib] / norm1 - w1f[...] * (dot_first / (norm1 * norm1 * norm1))
    mine = pl.ds(pl.multiple_of(z * ip, 128), ip)
    norm2 = jnp.sqrt(1.0 + s2[0, :1, mine] + s2[1, :1, mine])[:, :ib]
    dot_second = second[hb : hb + 1, :ib]
    out2[...] = second[:hb, :ib] / norm2 - w2f[...] * (dot_second / (norm2 * norm2 * norm2))
    for cond, spec in pending:
        when(cond, lambda spec=spec: remote(*spec).wait_send())


def local_step(clean, noise, bucket, mod_table, w_first, w_second):
    rows = lax.axis_size("row")
    cols = lax.axis_size("col")
    z, col = lax.axis_index("row"), lax.axis_index("col")
    samples = bucket.shape[0]
    own_rows = clean.shape[1]
    ib, hb = clean.shape[0], w_first.shape[2]
    sub = own_rows // rows
    if sub != PIX:
        return local(clean, noise, bucket, mod_table, w_first, w_second)
    chips = cols // CORES
    hp, ip = round_up(hb + 1, 16), round_up(ib + 1, 128)
    bf16 = jnp.bfloat16
    w1f, w2f = w_first[0].T, w_second[0]
    wown = jnp.stack([w1f, w2f]).astype(bf16)
    wown = jnp.pad(wown, ((0, 0), (0, hp - hb), (0, ip - ib)))
    sample = lax.dynamic_slice_in_dim(bucket, col * rows, rows)
    levels = jnp.repeat(noise_levels(sample), PIX)[None, :]
    root = jnp.sqrt(levels * levels + 0.25)
    sto = jnp.stack([
        ((clean + levels * noise) / root).astype(bf16),
        (clean * (2.0 * levels / root) - noise * (0.5 / root)).astype(bf16),
    ])
    chip = col // CORES
    picked = jnp.stack([lax.dynamic_index_in_dim(bucket, (chip * CORES + j) * rows + z, keepdims=False) for j in range(CORES)])
    table = mod_table[0].reshape(mod_table.shape[1], chips, CORES, hb)
    mine = lax.dynamic_index_in_dim(table, lax.rem(col, CORES), axis=2, keepdims=False)
    gsel = 1.0 + jnp.take(mine, picked, axis=0)
    gsel = jnp.pad(gsel, ((0, 0), (0, 0), (0, hp - hb))).reshape(CORES, chips * hp, 1)
    hh, ii = chips * hp, rows * ip
    f32 = jnp.float32
    vmem = pl.BlockSpec(memory_space=pltpu.VMEM)
    out1, out2 = pl.pallas_call(
        lambda *refs: step_kernel(hb, ib, samples, *refs),
        out_shape=(jax.ShapeDtypeStruct((hb, ib), f32), jax.ShapeDtypeStruct((hb, ib), f32)),
        in_specs=[vmem] * 5,
        out_specs=(vmem, vmem),
        scratch_shapes=[
            pltpu.VMEM((2, hh, ii), bf16),
            pltpu.VMEM((2, ii, sub), bf16),
            pltpu.VMEM((ii, sub), bf16),
            pltpu.VMEM((2, hh, sub), f32),
            pltpu.VMEM((2, hh, sub), bf16),
            pltpu.VMEM((ii, sub), f32),
            pltpu.VMEM((ii, sub), f32),
            pltpu.VMEM((ii, sub), f32),
            pltpu.VMEM((2, ii, sub), bf16),
            pltpu.VMEM((2, ii, sub), bf16),
            pltpu.VMEM((2, hh, sub), bf16),
            pltpu.VMEM((2, 8, ii), f32),
            pltpu.VMEM((2, 8, ii), f32),
            pltpu.VMEM((2, hh, ii), bf16),
            pltpu.VMEM((2, rows, hp, ip), bf16),
            pltpu.VMEM((2, rows, hp, ip), bf16),
            pltpu.VMEM((2, rows, hp, ip), bf16),
            pltpu.VMEM((2, rows, hp, ip), bf16),
            pltpu.VMEM((rows, 2, hp, ip), bf16),
            pltpu.VMEM((rows, 2, hp, ip), bf16),
            pltpu.VMEM((hh, 128), f32),
            pltpu.SemaphoreType.DMA((32, max(rows, 11))),
        ],
        compiler_params=pltpu.CompilerParams(
            collective_id=0, has_side_effects=True, vmem_limit_bytes=60 * 1024 * 1024
        ),
    )(wown, sto, gsel, w1f, w2f)
    return (out1.T[None], out2[None])


def solution(mesh):
    placed = (
        P("row", "col"),
        P("row", "col"),
        P(),
        P(),
        P(None, "row", "col"),
        P(None, "col", "row"),
    )
    return jax.shard_map(
        local_step if mesh.shape["col"] == CORES * SIDE * SIDE else local,
        mesh=mesh,
        in_specs=placed,
        out_specs=(P(None, "row", "col"), P(None, "col", "row")),
        check_vma=False,
    )
```

```python
import math

import jax
import jax.numpy as jnp
from jax import lax
from jax.experimental import pallas as pl
from jax.experimental.pallas import tpu as pltpu
from jax.sharding import PartitionSpec as P

PIX = 256
BUCKETS = 32


MIX_WEIGHT = 0.3
KEEP_COEF = (1.0 - MIX_WEIGHT) / math.sqrt((1.0 - MIX_WEIGHT) ** 2 + MIX_WEIGHT**2)
ADD_COEF = MIX_WEIGHT / math.sqrt((1.0 - MIX_WEIGHT) ** 2 + MIX_WEIGHT**2)
SILU_GAIN = 1.0 / 0.596
CONTRACT_LEAD = (((0,), (0,)), ((), ()))
CONTRACT_TAIL = (((1,), (1,)), ((), ()))


def noise_levels(bucket):
    return jnp.exp(-3.0 + 5.0 * (bucket.astype(jnp.float32) + 0.5) / BUCKETS)


def silu_slope(values):
    sig = jax.nn.sigmoid(values)
    return sig * (1.0 + values * (1.0 - sig))


def bucket_gains(table, picked):
    onehot = (picked[:, None] == jnp.arange(table.shape[0], dtype=jnp.int32)[None, :]).astype(
        jnp.float32
    )
    return jnp.dot(
        onehot, table, precision=lax.Precision.HIGHEST, preferred_element_type=jnp.float32
    )


def local(clean, noise, bucket, mod_table, w_first, w_second):
    rows_size = lax.axis_size("row")
    row_at = lax.axis_index("row")
    col_at = lax.axis_index("col")
    samples = bucket.shape[0]
    own_rows = clean.shape[1]
    weight_first = w_first[0]
    weight_second = w_second[0]
    table = 1.0 + mod_table[0]
    col_first = jnp.sqrt(lax.psum(jnp.sum(weight_first * weight_first, axis=0), "row") + 1.0)
    col_second = jnp.sqrt(lax.psum(jnp.sum(weight_second * weight_second, axis=0), "col") + 1.0)
    normed_first = (weight_first / col_first[None, :]).astype(jnp.bfloat16)
    normed_second = (weight_second / col_second[None, :]).astype(jnp.bfloat16)
    chan_clean, chan_noise = (
        lax.all_to_all(
            clean.astype(jnp.bfloat16), "row", split_axis=1, concat_axis=0, tiled=True
        ).astype(clean.dtype),
        lax.all_to_all(
            noise.astype(jnp.bfloat16), "row", split_axis=1, concat_axis=0, tiled=True
        ).astype(noise.dtype),
    )
    local_clean = chan_clean.T
    local_noise = chan_noise.T
    sub_rows = own_rows // rows_size
    first_row = col_at * own_rows + row_at * sub_rows
    row_sample = (first_row + jnp.arange(sub_rows, dtype=jnp.int32)) // PIX
    row_bucket = jnp.take(bucket, row_sample)
    levels = noise_levels(row_bucket)[:, None]
    spread_root = jnp.sqrt(levels * levels + 0.25)
    state_own = ((local_clean + levels * local_noise) / spread_root).astype(jnp.bfloat16)
    target = local_clean * (2.0 * levels / spread_root) - local_noise * (0.5 / spread_root)
    gains = bucket_gains(table, row_bucket)
    part_first, part_second = (
        lax.all_gather(normed_first, "col", axis=1, tiled=True),
        lax.all_gather(normed_second, "col", axis=0, tiled=True),
    )
    full_first, full_second = (
        lax.all_gather(part_first, "row", axis=0, tiled=True),
        lax.all_gather(part_second, "row", axis=1, tiled=True),
    )
    pre_act = jnp.dot(state_own, full_first, preferred_element_type=jnp.float32)
    hidden = (jax.nn.silu(pre_act) * SILU_GAIN * gains).astype(jnp.bfloat16)
    branch = jnp.dot(hidden, full_second, preferred_element_type=jnp.float32)
    state_new = (KEEP_COEF * state_own.astype(jnp.float32) + ADD_COEF * branch).astype(jnp.bfloat16)
    grad_own = (state_new.astype(jnp.float32) - target) / samples
    dbranch = (ADD_COEF * grad_own).astype(jnp.bfloat16)
    gsecond_full = lax.dot_general(
        hidden, dbranch, CONTRACT_LEAD, preferred_element_type=jnp.float32
    )
    dhidden = lax.dot_general(
        dbranch, full_second, CONTRACT_TAIL, preferred_element_type=jnp.float32
    )
    dpre = (dhidden * gains * silu_slope(pre_act) * SILU_GAIN).astype(jnp.bfloat16)
    gfirst_full = lax.dot_general(
        state_own, dpre, CONTRACT_LEAD, preferred_element_type=jnp.float32
    )
    part_gfirst, part_gsecond = (
        lax.psum_scatter(
            gfirst_full.astype(jnp.bfloat16), "col", scatter_dimension=1, tiled=True
        ).astype(jnp.float32),
        lax.psum_scatter(
            gsecond_full.astype(jnp.bfloat16), "col", scatter_dimension=0, tiled=True
        ).astype(jnp.float32),
    )
    gfirst, gsecond = (
        lax.psum_scatter(
            part_gfirst.astype(jnp.bfloat16), "row", scatter_dimension=0, tiled=True
        ).astype(jnp.float32),
        lax.psum_scatter(
            part_gsecond.astype(jnp.bfloat16), "row", scatter_dimension=1, tiled=True
        ).astype(jnp.float32),
    )
    dot_first = lax.psum(jnp.sum(weight_first * gfirst, axis=0), "row")
    dot_second = lax.psum(jnp.sum(weight_second * gsecond, axis=0), "col")
    grad_first = gfirst / col_first[None, :] - weight_first * (dot_first / col_first**3)[None, :]
    grad_second = (
        gsecond / col_second[None, :] - weight_second * (dot_second / col_second**3)[None, :]
    )
    return (grad_first[None], grad_second[None])


CORES = 2
SIDE = 2
MESH = pl.DeviceIdType.MESH
(S_UP, S_DN, S_X, S_Y, S_D0, S_D1, S_S, S_T, S_F, R_Z, R_X, R_Y, R_D0, R_D1, R_S, R_T, R_F,
 S_A0, S_A1, R_A0, R_A1, S_BX, S_CX, S_BY, S_CY, R_BX, R_CX, R_BY, R_CY, S_P, R_P, MISC) = range(32)


def round_up(size, unit):
    return -(-size // unit) * unit


def step_kernel(
    hb, ib, samples, wown, sto, gsel, w1f, w2f, out1, out2,
    w, st, tg, pre, hid, brp, brk, brr, dbr, db2, dpre, s2, d2, g,
    ra, sa, rx, ry, pz, rz, colf, gcol, sems,
):
    rows = st.shape[1] // wown.shape[2]
    hp, ip = wown.shape[1], wown.shape[2]
    chips = w.shape[1] // hp
    sub = st.shape[2]
    z = lax.axis_index("row")
    col = lax.axis_index("col")
    core = lax.rem(col, CORES)
    xy = col // CORES
    x, y = lax.rem(xy, SIDE), xy // SIDE
    xn = y * SIDE + (1 - x)
    yn = (1 - y) * SIDE + x
    dn = (1 - y) * SIDE + (1 - x)
    dev_x = (z, xn * CORES + core)
    dev_y = (z, yn * CORES + core)
    dev_p = (z, xy * CORES + 1 - core)
    up, down = (z + 1, col), (z - 1, col)
    ring = [lax.rem(z + k, rows) for k in range(rows)]

    barrier = pltpu.get_barrier_semaphore()
    peers = [dev_x, dev_y, dev_p] + [(ring[k], col) for k in range(1, rows)]
    for peer in peers:
        pl.semaphore_signal(barrier, inc=1, device_id=peer, device_id_type=MESH)

    pending = []

    def remote(src, dst, send, recv, dev):
        return pltpu.make_async_remote_copy(
            src_ref=src, dst_ref=dst, send_sem=sems.at[send[0], send[1]],
            recv_sem=sems.at[recv[0], recv[1]], device_id=dev, device_id_type=MESH,
        )

    def when(cond, fn):
        if cond is None:
            fn()
        else:
            pl.when(cond)(fn)

    def send(cond, *spec):
        when(cond, lambda: remote(*spec).start())
        pending.append((cond, spec))

    def arrive(cond, dst, recv):
        when(cond, lambda: remote(dst, dst, recv, recv, dev_p).wait_recv())

    def both(a, b):
        return b if a is None else (a if b is None else jnp.logical_and(a, b))

    def blk(zb, xyb, half=None):
        at = (pl.ds(pl.multiple_of(xyb * hp, 16), hp), pl.ds(pl.multiple_of(zb * ip, 128), ip))
        return w.at[(slice(None),) + at] if half is None else w.at[(half,) + at]

    def chan(zb):
        return pl.ds(pl.multiple_of(zb * ip, 128), ib)

    def pix(zb):
        return pl.ds(pl.multiple_of(zb * sub, 128), sub)

    local_w = pltpu.make_async_copy(wown, blk(z, xy), sems.at[MISC, 0])
    local_w.start()
    local_s = pltpu.make_async_copy(sto.at[0, :, pix(z)], st.at[core, chan(z)], sems.at[MISC, 1])
    local_s.start()
    local_t = pltpu.make_async_copy(sto.at[1, :, pix(z)], tg.at[chan(z)], sems.at[MISC, 2])
    local_t.start()
    for zb in range(rows):
        pad = slice(zb * ip + ib, (zb + 1) * ip)
        zero = jnp.zeros((ip - ib, sub), jnp.bfloat16)
        st[0, pad, :] = zero
        st[1, pad, :] = zero
        tg[pad, :] = zero
    pl.semaphore_wait(barrier, len(peers))

    def spread(cond, zb, src, go_up, go_down):
        if go_up:
            send(both(cond, z + 1 < rows), src, blk(zb, xy), (S_UP, zb), (R_Z, zb), up)
        if go_down:
            send(both(cond, z > 0), src, blk(zb, xy), (S_DN, zb), (R_Z, zb), down)
        send(cond, src, blk(zb, xy), (S_X, zb), (R_X, zb), dev_x)
        send(cond, src, blk(zb, xy), (S_Y, zb), (R_Y, zb), dev_y)

    def state_out(k):
        zt = ring[k]
        send(None, sto.at[0, :, pix(zt)], st.at[core, chan(z)], (S_S, k), (R_S, z), (zt, col))

    def diagonal(cond, zb):
        arrive(cond, blk(zb, xn), (R_X, zb))
        send(cond, blk(zb, xn, 0), blk(zb, xn, 0), (S_D0, zb), (R_D0, zb), dev_y)
        arrive(cond, blk(zb, yn), (R_Y, zb))
        send(cond, blk(zb, yn, 1), blk(zb, yn, 1), (S_D1, zb), (R_D1, zb), dev_x)

    spread(None, z, wown, True, True)
    send(None, sto.at[0, :, pix(z)], st.at[core, chan(z)], (S_F, z), (R_F, z), dev_p)
    for k in range(1, rows):
        state_out(k)
    for d in range(1, rows + 1):
        if d < rows:
            low, high = z - d, z + d
            arrive(low >= 0, blk(low, xy), (R_Z, low))
            spread(low >= 0, low, blk(low, xy), True, False)
            arrive(high < rows, blk(high, xy), (R_Z, high))
            spread(high < rows, high, blk(high, xy), False, True)
        if d == 1:
            for k in range(1, rows):
                zt = ring[k]
                send(None, sto.at[1, :, pix(zt)], tg.at[chan(z)], (S_T, k), (R_T, z), (zt, col))
        if d == 1:
            diagonal(None, z)
        else:
            diagonal(z - (d - 1) >= 0, z - (d - 1))
            diagonal(z + (d - 1) < rows, z + (d - 1))
    for k in range(1, rows):
        zb = ring[rows - k]
        arrive(None, st.at[core, chan(zb)], (R_S, zb))
        send(None, st.at[core, chan(zb)], st.at[core, chan(zb)], (S_F, zb), (R_F, zb), dev_p)
    for zb in range(rows):
        arrive(None, blk(zb, dn, 0), (R_D0, zb))
        arrive(None, blk(zb, dn, 1), (R_D1, zb))
    local_w.wait()
    local_s.wait()
    local_t.wait()

    half_rows = w.shape[1] // 2
    for j in range(CORES):
        gcol[j] = gsel[j].T
    for part in range(2):
        at = slice(part * half_rows, (part + 1) * half_rows)
        block = w[0, at, :].astype(jnp.float32)
        colf[at, :] = jnp.broadcast_to(
            jnp.sqrt(1.0 + jnp.sum(block * block, axis=1, keepdims=True)), (half_rows, colf.shape[1])
        )
    total = jnp.zeros((1, w.shape[2]), jnp.float32)
    for part in range(2):
        block = w[1, part * half_rows : (part + 1) * half_rows, :].astype(jnp.float32)
        total = total + jnp.sum(block * block, axis=0, keepdims=True)
    s2[0] = jnp.broadcast_to(total, s2.shape[1:])
    send(None, s2.at[0], s2.at[1], (MISC, 3), (MISC, 4), dev_p)
    for zb in range(rows):
        arrive(None, st.at[1 - core, chan(zb)], (R_F, zb))

    def forward(j):
        @pl.loop(0, 2)
        def _(part):
            at = pl.ds(pl.multiple_of(part * half_rows, 16), half_rows)
            value = jnp.dot(w[0, at, :], st[j], preferred_element_type=jnp.float32)
            value = value / colf[at, :1]
            pre[j, at, :] = value
            hid[j, at, :] = (value * jax.nn.sigmoid(value) * SILU_GAIN * gcol[j, at, :1]).astype(jnp.bfloat16)

    def branch_part(j, dst):
        @pl.loop(0, rows)
        def _(zb):
            at = pl.ds(pl.multiple_of(zb * ip, 128), ip)
            dst[at, :] = lax.dot_general(
                w[1, :, at], hid[j], CONTRACT_LEAD, preferred_element_type=jnp.float32
            )

    forward(1 - core)
    branch_part(1 - core, brp)
    send(None, brp, brr, (MISC, 5), (MISC, 6), dev_p)
    forward(core)
    branch_part(core, brk)
    for k in range(1, rows):
        arrive(None, tg.at[chan(ring[k])], (R_T, ring[k]))
    arrive(None, s2.at[1], (MISC, 4))
    col2_row = jnp.sqrt(1.0 + s2[0] + s2[1])
    col2 = col2_row.T[:, :1]
    arrive(None, brr, (MISC, 6))
    for zb in range(rows):
        at = slice(zb * ip, (zb + 1) * ip)
        norm = col2[at, :]
        branch = (brk[at, :] + brr[at, :]) / norm
        fresh = (KEEP_COEF * st[core, at, :].astype(jnp.float32) + ADD_COEF * branch).astype(jnp.bfloat16)
        slope = (fresh.astype(jnp.float32) - tg[at, :].astype(jnp.float32)) / samples
        rounded = (ADD_COEF * slope).astype(jnp.bfloat16)
        dbr[core, at, :] = rounded
        product = jnp.sum(branch * rounded.astype(jnp.float32), axis=1, keepdims=True) * norm
        d2[0, :, at] = jnp.broadcast_to(product, (ip, 128)).T[: d2.shape[1], :]
    send(None, dbr.at[core], dbr.at[core], (MISC, 7), (MISC, 8), dev_p)
    send(None, d2.at[0], d2.at[1], (MISC, 9), (MISC, 10), dev_p)

    def scale_back(j):
        for zb in range(rows):
            at = slice(zb * ip, (zb + 1) * ip)
            db2[j, at, :] = (dbr[j, at, :].astype(jnp.float32) / col2[at, :]).astype(jnp.bfloat16)

    def backward(j):
        @pl.loop(0, 2)
        def _(part):
            at = pl.ds(pl.multiple_of(part * half_rows, 16), half_rows)
            grad = jnp.dot(w[1, at, :], db2[j], preferred_element_type=jnp.float32)
            dpre[j, at, :] = (grad * gcol[j, at, :1] * silu_slope(pre[j, at, :]) * SILU_GAIN).astype(jnp.bfloat16)

    scale_back(core)
    backward(core)
    arrive(None, dbr.at[1 - core], (MISC, 8))
    arrive(None, d2.at[1], (MISC, 10))
    lane = lax.broadcasted_iota(jnp.int32, (1, ip), 1)
    line = lax.broadcasted_iota(jnp.int32, (hp, 1), 0)
    order = ring[1:] + ring[:1]

    def gblk(half, xyb, zb):
        return (half, pl.ds(pl.multiple_of(xyb * hp, 16), hp), pl.ds(pl.multiple_of(zb * ip, 128), ip))

    def wide(value):
        return value.astype(jnp.float32)

    for k in range(rows):
        at = pl.ds(pl.multiple_of(order[k] * ip, 128), ip)
        second = sum(
            lax.dot_general(hid[j], dbr[j, at, :], CONTRACT_TAIL, preferred_element_type=jnp.float32)
            for j in range(CORES)
        )
        dot2 = d2[0, :1, at] + d2[1, :1, at]
        for b in range(chips):
            part = second[b * hp : (b + 1) * hp, :]
            g[1, b * hp : (b + 1) * hp, at] = jnp.where(line >= hb, dot2, part).astype(jnp.bfloat16)
        send(None, g.at[gblk(1, dn, order[k])], ra.at[1, k], (S_A1, k), (R_A1, k), dev_x)
    for k in range(rows):
        send(None, g.at[gblk(1, xn, order[k])], rx.at[1, k], (S_CX, k), (R_CX, k), dev_x)
    scale_back(1 - core)
    backward(1 - core)
    dot1 = colf[:, :1] * sum(
        jnp.sum(dpre[j].astype(jnp.float32) * pre[j], axis=1, keepdims=True) for j in range(CORES)
    )

    def stage_a(k):
        zb = order[k]
        at = pl.ds(pl.multiple_of(zb * ip, 128), ip)
        first = sum(
            lax.dot_general(dpre[j], st[j, at, :], CONTRACT_TAIL, preferred_element_type=jnp.float32)
            for j in range(CORES)
        )
        g[0, :, at] = jnp.where(lane >= ib, dot1, first).astype(jnp.bfloat16)
        send(None, g.at[gblk(0, dn, zb)], ra.at[0, k], (S_A0, k), (R_A0, k), dev_y)
        arrive(None, ra.at[1, k], (R_A1, k))
        sa[1, k] = (wide(g[gblk(1, yn, zb)]) + wide(ra[1, k])).astype(jnp.bfloat16)
        send(None, sa.at[1, k], ry.at[1, k], (S_BY, k), (R_BY, k), dev_y)
        send(None, g.at[gblk(0, yn, zb)], ry.at[0, k], (S_CY, k), (R_CY, k), dev_y)

    def stage_b(k):
        zb = order[k]
        arrive(None, ra.at[0, k], (R_A0, k))
        sa[0, k] = (wide(g[gblk(0, xn, zb)]) + wide(ra[0, k])).astype(jnp.bfloat16)
        send(None, sa.at[0, k], rx.at[0, k], (S_BX, k), (R_BX, k), dev_x)

    def stage_c(k):
        zb = order[k]
        arrive(None, rx.at[1, k], (R_CX, k))
        arrive(None, ry.at[0, k], (R_CY, k))
        arrive(None, rx.at[0, k], (R_BX, k))
        arrive(None, ry.at[1, k], (R_BY, k))
        sums = [wide(g[gblk(half, xy, zb)]) + wide(rx[half, k]) + wide(ry[half, k]) for half in range(2)]
        if k == rows - 1:
            return sums
        pz[k, 0] = sums[0].astype(jnp.bfloat16)
        pz[k, 1] = sums[1].astype(jnp.bfloat16)
        send(None, pz.at[k], rz.at[k], (S_P, k), (R_P, k), (zb, col))
        return None

    for k in range(rows):
        stage_a(k)
        if k >= 1:
            stage_b(k - 1)
    sums = None
    for k in range(rows):
        if k == rows - 2:
            stage_b(rows - 1)
        sums = stage_c(k)
    for k in range(rows - 1):
        arrive(None, rz.at[k], (R_P, k))
    first, second = (
        sums[half] + sum(wide(rz[k, half]) for k in range(rows - 1)) for half in range(2)
    )
    norm1 = colf[pl.ds(pl.multiple_of(xy * hp, 16), hp), :1][:hb]
    dot_first = first[:hb, ib : ib + 1]
    out1[...] = first[:hb, :ib] / norm1 - w1f[...] * (dot_first / (norm1 * norm1 * norm1))
    mine = pl.ds(pl.multiple_of(z * ip, 128), ip)
    norm2 = jnp.sqrt(1.0 + s2[0, :1, mine] + s2[1, :1, mine])[:, :ib]
    dot_second = second[hb : hb + 1, :ib]
    out2[...] = second[:hb, :ib] / norm2 - w2f[...] * (dot_second / (norm2 * norm2 * norm2))
    for cond, spec in pending:
        when(cond, lambda spec=spec: remote(*spec).wait_send())


def local_step(clean, noise, bucket, mod_table, w_first, w_second):
    rows = lax.axis_size("row")
    cols = lax.axis_size("col")
    z, col = lax.axis_index("row"), lax.axis_index("col")
    samples = bucket.shape[0]
    own_rows = clean.shape[1]
    ib, hb = clean.shape[0], w_first.shape[2]
    sub = own_rows // rows
    if sub != PIX:
        return local(clean, noise, bucket, mod_table, w_first, w_second)
    chips = cols // CORES
    hp, ip = round_up(hb + 1, 16), round_up(ib + 1, 128)
    bf16 = jnp.bfloat16
    w1f, w2f = w_first[0].T, w_second[0]
    wown = jnp.stack([w1f, w2f]).astype(bf16)
    wown = jnp.pad(wown, ((0, 0), (0, hp - hb), (0, ip - ib)))
    sample = lax.dynamic_slice_in_dim(bucket, col * rows, rows)
    levels = jnp.repeat(noise_levels(sample), PIX)[None, :]
    root = jnp.sqrt(levels * levels + 0.25)
    sto = jnp.stack([
        ((clean + levels * noise) / root).astype(bf16),
        (clean * (2.0 * levels / root) - noise * (0.5 / root)).astype(bf16),
    ])
    chip = col // CORES
    table = mod_table.reshape(mod_table.shape[1], chips, CORES, hb)
    picked = [
        lax.dynamic_slice(
            table, (bucket[(chip * CORES + j) * rows + z], 0, lax.rem(col, CORES), 0), (1, chips, 1, hb)
        )[0, :, 0]
        for j in range(CORES)
    ]
    gsel = jnp.pad(1.0 + jnp.stack(picked), ((0, 0), (0, 0), (0, hp - hb)))
    gsel = jnp.broadcast_to(gsel.reshape(CORES, 1, chips * hp), (CORES, 8, chips * hp))
    hh, ii = chips * hp, rows * ip
    f32 = jnp.float32
    vmem = pl.BlockSpec(memory_space=pltpu.VMEM)
    out1, out2 = pl.pallas_call(
        lambda *refs: step_kernel(hb, ib, samples, *refs),
        out_shape=(jax.ShapeDtypeStruct((hb, ib), f32), jax.ShapeDtypeStruct((hb, ib), f32)),
        in_specs=[vmem] * 5,
        out_specs=(vmem, vmem),
        scratch_shapes=[
            pltpu.VMEM((2, hh, ii), bf16),
            pltpu.VMEM((2, ii, sub), bf16),
            pltpu.VMEM((ii, sub), bf16),
            pltpu.VMEM((2, hh, sub), f32),
            pltpu.VMEM((2, hh, sub), bf16),
            pltpu.VMEM((ii, sub), f32),
            pltpu.VMEM((ii, sub), f32),
            pltpu.VMEM((ii, sub), f32),
            pltpu.VMEM((2, ii, sub), bf16),
            pltpu.VMEM((2, ii, sub), bf16),
            pltpu.VMEM((2, hh, sub), bf16),
            pltpu.VMEM((2, 8, ii), f32),
            pltpu.VMEM((2, 8, ii), f32),
            pltpu.VMEM((2, hh, ii), bf16),
            pltpu.VMEM((2, rows, hp, ip), bf16),
            pltpu.VMEM((2, rows, hp, ip), bf16),
            pltpu.VMEM((2, rows, hp, ip), bf16),
            pltpu.VMEM((2, rows, hp, ip), bf16),
            pltpu.VMEM((rows, 2, hp, ip), bf16),
            pltpu.VMEM((rows, 2, hp, ip), bf16),
            pltpu.VMEM((hh, 128), f32),
            pltpu.VMEM((CORES, hh, 8), f32),
            pltpu.SemaphoreType.DMA((32, max(rows, 11))),
        ],
        compiler_params=pltpu.CompilerParams(
            collective_id=0, has_side_effects=True, vmem_limit_bytes=60 * 1024 * 1024
        ),
    )(wown, sto, gsel, w1f, w2f)
    return (out1.T[None], out2[None])


def solution(mesh):
    placed = (
        P("row", "col"),
        P("row", "col"),
        P(),
        P(),
        P(None, "row", "col"),
        P(None, "col", "row"),
    )
    return jax.shard_map(
        local_step if mesh.shape["col"] == CORES * SIDE * SIDE else local,
        mesh=mesh,
        in_specs=placed,
        out_specs=(P(None, "row", "col"), P(None, "col", "row")),
        check_vma=False,
    )
```

```python
import math

import jax
import jax.numpy as jnp
from jax import lax
from jax.experimental import pallas as pl
from jax.experimental.pallas import tpu as pltpu
from jax.sharding import PartitionSpec as P

PIX = 256
BUCKETS = 32


MIX_WEIGHT = 0.3
KEEP_COEF = (1.0 - MIX_WEIGHT) / math.sqrt((1.0 - MIX_WEIGHT) ** 2 + MIX_WEIGHT**2)
ADD_COEF = MIX_WEIGHT / math.sqrt((1.0 - MIX_WEIGHT) ** 2 + MIX_WEIGHT**2)
SILU_GAIN = 1.0 / 0.596
CONTRACT_LEAD = (((0,), (0,)), ((), ()))
CONTRACT_TAIL = (((1,), (1,)), ((), ()))


def noise_levels(bucket):
    return jnp.exp(-3.0 + 5.0 * (bucket.astype(jnp.float32) + 0.5) / BUCKETS)


def silu_slope(values):
    sig = jax.nn.sigmoid(values)
    return sig * (1.0 + values * (1.0 - sig))


def bucket_gains(table, picked):
    onehot = (picked[:, None] == jnp.arange(table.shape[0], dtype=jnp.int32)[None, :]).astype(
        jnp.float32
    )
    return jnp.dot(
        onehot, table, precision=lax.Precision.HIGHEST, preferred_element_type=jnp.float32
    )


def local(clean, noise, bucket, mod_table, w_first, w_second):
    rows_size = lax.axis_size("row")
    row_at = lax.axis_index("row")
    col_at = lax.axis_index("col")
    samples = bucket.shape[0]
    own_rows = clean.shape[1]
    weight_first = w_first[0]
    weight_second = w_second[0]
    table = 1.0 + mod_table[0]
    col_first = jnp.sqrt(lax.psum(jnp.sum(weight_first * weight_first, axis=0), "row") + 1.0)
    col_second = jnp.sqrt(lax.psum(jnp.sum(weight_second * weight_second, axis=0), "col") + 1.0)
    normed_first = (weight_first / col_first[None, :]).astype(jnp.bfloat16)
    normed_second = (weight_second / col_second[None, :]).astype(jnp.bfloat16)
    chan_clean, chan_noise = (
        lax.all_to_all(
            clean.astype(jnp.bfloat16), "row", split_axis=1, concat_axis=0, tiled=True
        ).astype(clean.dtype),
        lax.all_to_all(
            noise.astype(jnp.bfloat16), "row", split_axis=1, concat_axis=0, tiled=True
        ).astype(noise.dtype),
    )
    local_clean = chan_clean.T
    local_noise = chan_noise.T
    sub_rows = own_rows // rows_size
    first_row = col_at * own_rows + row_at * sub_rows
    row_sample = (first_row + jnp.arange(sub_rows, dtype=jnp.int32)) // PIX
    row_bucket = jnp.take(bucket, row_sample)
    levels = noise_levels(row_bucket)[:, None]
    spread_root = jnp.sqrt(levels * levels + 0.25)
    state_own = ((local_clean + levels * local_noise) / spread_root).astype(jnp.bfloat16)
    target = local_clean * (2.0 * levels / spread_root) - local_noise * (0.5 / spread_root)
    gains = bucket_gains(table, row_bucket)
    part_first, part_second = (
        lax.all_gather(normed_first, "col", axis=1, tiled=True),
        lax.all_gather(normed_second, "col", axis=0, tiled=True),
    )
    full_first, full_second = (
        lax.all_gather(part_first, "row", axis=0, tiled=True),
        lax.all_gather(part_second, "row", axis=1, tiled=True),
    )
    pre_act = jnp.dot(state_own, full_first, preferred_element_type=jnp.float32)
    hidden = (jax.nn.silu(pre_act) * SILU_GAIN * gains).astype(jnp.bfloat16)
    branch = jnp.dot(hidden, full_second, preferred_element_type=jnp.float32)
    state_new = (KEEP_COEF * state_own.astype(jnp.float32) + ADD_COEF * branch).astype(jnp.bfloat16)
    grad_own = (state_new.astype(jnp.float32) - target) / samples
    dbranch = (ADD_COEF * grad_own).astype(jnp.bfloat16)
    gsecond_full = lax.dot_general(
        hidden, dbranch, CONTRACT_LEAD, preferred_element_type=jnp.float32
    )
    dhidden = lax.dot_general(
        dbranch, full_second, CONTRACT_TAIL, preferred_element_type=jnp.float32
    )
    dpre = (dhidden * gains * silu_slope(pre_act) * SILU_GAIN).astype(jnp.bfloat16)
    gfirst_full = lax.dot_general(
        state_own, dpre, CONTRACT_LEAD, preferred_element_type=jnp.float32
    )
    part_gfirst, part_gsecond = (
        lax.psum_scatter(
            gfirst_full.astype(jnp.bfloat16), "col", scatter_dimension=1, tiled=True
        ).astype(jnp.float32),
        lax.psum_scatter(
            gsecond_full.astype(jnp.bfloat16), "col", scatter_dimension=0, tiled=True
        ).astype(jnp.float32),
    )
    gfirst, gsecond = (
        lax.psum_scatter(
            part_gfirst.astype(jnp.bfloat16), "row", scatter_dimension=0, tiled=True
        ).astype(jnp.float32),
        lax.psum_scatter(
            part_gsecond.astype(jnp.bfloat16), "row", scatter_dimension=1, tiled=True
        ).astype(jnp.float32),
    )
    dot_first = lax.psum(jnp.sum(weight_first * gfirst, axis=0), "row")
    dot_second = lax.psum(jnp.sum(weight_second * gsecond, axis=0), "col")
    grad_first = gfirst / col_first[None, :] - weight_first * (dot_first / col_first**3)[None, :]
    grad_second = (
        gsecond / col_second[None, :] - weight_second * (dot_second / col_second**3)[None, :]
    )
    return (grad_first[None], grad_second[None])


CORES = 2
SIDE = 2
MESH = pl.DeviceIdType.MESH
(S_UP, S_DN, S_X, S_Y, S_D0, S_D1, S_S, S_T, S_F, R_Z, R_X, R_Y, R_D0, R_D1, R_S, R_T, R_F,
 S_A0, S_A1, R_A0, R_A1, S_BX, S_CX, S_BY, S_CY, R_BX, R_CX, R_BY, R_CY, S_P, R_P, MISC) = range(32)


def round_up(size, unit):
    return -(-size // unit) * unit


def step_kernel(
    hb, ib, samples, wown, sto, gsel, w1f, w2f, out1, out2,
    w, st, tg, pre, hid, brp, brk, brr, dbr, db2, dpre, s2, d2, g,
    ra, sa, rx, ry, pz, rz, colf, sems,
):
    rows = st.shape[1] // wown.shape[2]
    hp, ip = wown.shape[1], wown.shape[2]
    chips = w.shape[1] // hp
    sub = st.shape[2]
    z = lax.axis_index("row")
    col = lax.axis_index("col")
    core = lax.rem(col, CORES)
    xy = col // CORES
    x, y = lax.rem(xy, SIDE), xy // SIDE
    xn = y * SIDE + (1 - x)
    yn = (1 - y) * SIDE + x
    dn = (1 - y) * SIDE + (1 - x)
    dev_x = (z, xn * CORES + core)
    dev_y = (z, yn * CORES + core)
    dev_p = (z, xy * CORES + 1 - core)
    up, down = (z + 1, col), (z - 1, col)
    ring = [lax.rem(z + k, rows) for k in range(rows)]

    barrier = pltpu.get_barrier_semaphore()
    peers = [dev_x, dev_y, dev_p] + [(ring[k], col) for k in range(1, rows)]
    for peer in peers:
        pl.semaphore_signal(barrier, inc=1, device_id=peer, device_id_type=MESH)

    pending = []

    def remote(src, dst, send, recv, dev):
        return pltpu.make_async_remote_copy(
            src_ref=src, dst_ref=dst, send_sem=sems.at[send[0], send[1]],
            recv_sem=sems.at[recv[0], recv[1]], device_id=dev, device_id_type=MESH,
        )

    def when(cond, fn):
        if cond is None:
            fn()
        else:
            pl.when(cond)(fn)

    def send(cond, *spec):
        when(cond, lambda: remote(*spec).start())
        pending.append((cond, spec))

    def arrive(cond, dst, recv):
        when(cond, lambda: remote(dst, dst, recv, recv, dev_p).wait_recv())

    def both(a, b):
        return b if a is None else (a if b is None else jnp.logical_and(a, b))

    def blk(zb, xyb, half=None):
        at = (pl.ds(pl.multiple_of(xyb * hp, 16), hp), pl.ds(pl.multiple_of(zb * ip, 128), ip))
        return w.at[(slice(None),) + at] if half is None else w.at[(half,) + at]

    def chan(zb):
        return pl.ds(pl.multiple_of(zb * ip, 128), ib)

    def pix(zb):
        return pl.ds(pl.multiple_of(zb * sub, 128), sub)

    local_w = pltpu.make_async_copy(wown, blk(z, xy), sems.at[MISC, 0])
    local_w.start()
    local_s = pltpu.make_async_copy(sto.at[0, :, pix(z)], st.at[core, chan(z)], sems.at[MISC, 1])
    local_s.start()
    local_t = pltpu.make_async_copy(sto.at[1, :, pix(z)], tg.at[chan(z)], sems.at[MISC, 2])
    local_t.start()
    for zb in range(rows):
        pad = slice(zb * ip + ib, (zb + 1) * ip)
        zero = jnp.zeros((ip - ib, sub), jnp.bfloat16)
        st[0, pad, :] = zero
        st[1, pad, :] = zero
        tg[pad, :] = zero
    pl.semaphore_wait(barrier, len(peers))

    def spread(cond, zb, src, go_up, go_down):
        if go_up:
            send(both(cond, z + 1 < rows), src, blk(zb, xy), (S_UP, zb), (R_Z, zb), up)
        if go_down:
            send(both(cond, z > 0), src, blk(zb, xy), (S_DN, zb), (R_Z, zb), down)
        send(cond, src, blk(zb, xy), (S_X, zb), (R_X, zb), dev_x)
        send(cond, src, blk(zb, xy), (S_Y, zb), (R_Y, zb), dev_y)

    def state_out(k):
        zt = ring[k]
        send(None, sto.at[0, :, pix(zt)], st.at[core, chan(z)], (S_S, k), (R_S, z), (zt, col))

    def diagonal(cond, zb):
        arrive(cond, blk(zb, xn), (R_X, zb))
        send(cond, blk(zb, xn, 0), blk(zb, xn, 0), (S_D0, zb), (R_D0, zb), dev_y)
        arrive(cond, blk(zb, yn), (R_Y, zb))
        send(cond, blk(zb, yn, 1), blk(zb, yn, 1), (S_D1, zb), (R_D1, zb), dev_x)

    spread(None, z, wown, True, True)
    send(None, sto.at[0, :, pix(z)], st.at[core, chan(z)], (S_F, z), (R_F, z), dev_p)
    for d in range(1, rows + 1):
        if d < rows:
            low, high = z - d, z + d
            arrive(low >= 0, blk(low, xy), (R_Z, low))
            spread(low >= 0, low, blk(low, xy), True, False)
            arrive(high < rows, blk(high, xy), (R_Z, high))
            spread(high < rows, high, blk(high, xy), False, True)
        if d == rows - 2:
            for k in range(1, rows):
                state_out(k)
        if d == rows - 1:
            for k in range(1, rows):
                zt = ring[k]
                send(None, sto.at[1, :, pix(zt)], tg.at[chan(z)], (S_T, k), (R_T, z), (zt, col))
        if d == 1:
            diagonal(None, z)
        else:
            diagonal(z - (d - 1) >= 0, z - (d - 1))
            diagonal(z + (d - 1) < rows, z + (d - 1))
    for k in range(1, rows):
        zb = ring[rows - k]
        arrive(None, st.at[core, chan(zb)], (R_S, zb))
        send(None, st.at[core, chan(zb)], st.at[core, chan(zb)], (S_F, zb), (R_F, zb), dev_p)
    for zb in range(rows):
        arrive(None, blk(zb, dn, 0), (R_D0, zb))
        arrive(None, blk(zb, dn, 1), (R_D1, zb))
    local_w.wait()
    local_s.wait()
    local_t.wait()

    half_rows = w.shape[1] // 2
    for part in range(2):
        at = slice(part * half_rows, (part + 1) * half_rows)
        block = w[0, at, :].astype(jnp.float32)
        colf[at, :] = jnp.broadcast_to(
            jnp.sqrt(1.0 + jnp.sum(block * block, axis=1, keepdims=True)), (half_rows, colf.shape[1])
        )
    total = jnp.zeros((1, w.shape[2]), jnp.float32)
    for part in range(2):
        block = w[1, part * half_rows : (part + 1) * half_rows, :].astype(jnp.float32)
        total = total + jnp.sum(block * block, axis=0, keepdims=True)
    s2[0] = jnp.broadcast_to(total, s2.shape[1:])
    send(None, s2.at[0], s2.at[1], (MISC, 3), (MISC, 4), dev_p)
    for zb in range(rows):
        arrive(None, st.at[1 - core, chan(zb)], (R_F, zb))

    def forward(j):
        @pl.loop(0, 2)
        def _(part):
            at = pl.ds(pl.multiple_of(part * half_rows, 16), half_rows)
            value = jnp.dot(w[0, at, :], st[j], preferred_element_type=jnp.float32)
            value = value / colf[at, :1]
            pre[j, at, :] = value
            hid[j, at, :] = (value * jax.nn.sigmoid(value) * SILU_GAIN * gsel[j, at, :]).astype(jnp.bfloat16)

    def branch_part(j, dst):
        @pl.loop(0, rows)
        def _(zb):
            at = pl.ds(pl.multiple_of(zb * ip, 128), ip)
            dst[at, :] = lax.dot_general(
                w[1, :, at], hid[j], CONTRACT_LEAD, preferred_element_type=jnp.float32
            )

    forward(1 - core)
    branch_part(1 - core, brp)
    send(None, brp, brr, (MISC, 5), (MISC, 6), dev_p)
    forward(core)
    branch_part(core, brk)
    for k in range(1, rows):
        arrive(None, tg.at[chan(ring[k])], (R_T, ring[k]))
    arrive(None, s2.at[1], (MISC, 4))
    col2_row = jnp.sqrt(1.0 + s2[0] + s2[1])
    col2 = col2_row.T[:, :1]
    arrive(None, brr, (MISC, 6))
    for zb in range(rows):
        at = slice(zb * ip, (zb + 1) * ip)
        norm = col2[at, :]
        branch = (brk[at, :] + brr[at, :]) / norm
        fresh = (KEEP_COEF * st[core, at, :].astype(jnp.float32) + ADD_COEF * branch).astype(jnp.bfloat16)
        slope = (fresh.astype(jnp.float32) - tg[at, :].astype(jnp.float32)) / samples
        rounded = (ADD_COEF * slope).astype(jnp.bfloat16)
        dbr[core, at, :] = rounded
        product = jnp.sum(branch * rounded.astype(jnp.float32), axis=1, keepdims=True) * norm
        d2[0, :, at] = jnp.broadcast_to(product, (ip, 128)).T[: d2.shape[1], :]
    send(None, dbr.at[core], dbr.at[core], (MISC, 7), (MISC, 8), dev_p)
    send(None, d2.at[0], d2.at[1], (MISC, 9), (MISC, 10), dev_p)

    def scale_back(j):
        for zb in range(rows):
            at = slice(zb * ip, (zb + 1) * ip)
            db2[j, at, :] = (dbr[j, at, :].astype(jnp.float32) / col2[at, :]).astype(jnp.bfloat16)

    def backward(j):
        @pl.loop(0, 2)
        def _(part):
            at = pl.ds(pl.multiple_of(part * half_rows, 16), half_rows)
            grad = jnp.dot(w[1, at, :], db2[j], preferred_element_type=jnp.float32)
            dpre[j, at, :] = (grad * gsel[j, at, :] * silu_slope(pre[j, at, :]) * SILU_GAIN).astype(jnp.bfloat16)

    scale_back(core)
    backward(core)
    arrive(None, dbr.at[1 - core], (MISC, 8))
    arrive(None, d2.at[1], (MISC, 10))
    scale_back(1 - core)
    backward(1 - core)
    dot1 = colf[:, :1] * sum(
        jnp.sum(dpre[j].astype(jnp.float32) * pre[j], axis=1, keepdims=True) for j in range(CORES)
    )
    lane = lax.broadcasted_iota(jnp.int32, (1, ip), 1)
    line = lax.broadcasted_iota(jnp.int32, (hp, 1), 0)

    def gradients(zb):
        at = pl.ds(pl.multiple_of(zb * ip, 128), ip)
        first = sum(
            lax.dot_general(dpre[j], st[j, at, :], CONTRACT_TAIL, preferred_element_type=jnp.float32)
            for j in range(CORES)
        )
        g[0, :, at] = jnp.where(lane >= ib, dot1, first).astype(jnp.bfloat16)
        second = sum(
            lax.dot_general(hid[j], dbr[j, at, :], CONTRACT_TAIL, preferred_element_type=jnp.float32)
            for j in range(CORES)
        )
        dot2 = d2[0, :1, at] + d2[1, :1, at]
        for b in range(chips):
            part = second[b * hp : (b + 1) * hp, :]
            g[1, b * hp : (b + 1) * hp, at] = jnp.where(line >= hb, dot2, part).astype(jnp.bfloat16)

    def gblk(half, xyb, zb):
        return (half, pl.ds(pl.multiple_of(xyb * hp, 16), hp), pl.ds(pl.multiple_of(zb * ip, 128), ip))

    order = ring[1:] + ring[:1]

    def stage_a(k):
        zb = order[k]
        send(None, g.at[gblk(0, dn, zb)], ra.at[0, k], (S_A0, k), (R_A0, k), dev_y)
        send(None, g.at[gblk(1, dn, zb)], ra.at[1, k], (S_A1, k), (R_A1, k), dev_x)
        send(None, g.at[gblk(1, xn, zb)], rx.at[1, k], (S_CX, k), (R_CX, k), dev_x)
        send(None, g.at[gblk(0, yn, zb)], ry.at[0, k], (S_CY, k), (R_CY, k), dev_y)

    def wide(value):
        return value.astype(jnp.float32)

    def stage_b(k):
        zb = order[k]
        arrive(None, ra.at[0, k], (R_A0, k))
        sa[0, k] = (wide(g[gblk(0, xn, zb)]) + wide(ra[0, k])).astype(jnp.bfloat16)
        send(None, sa.at[0, k], rx.at[0, k], (S_BX, k), (R_BX, k), dev_x)
        arrive(None, ra.at[1, k], (R_A1, k))
        sa[1, k] = (wide(g[gblk(1, yn, zb)]) + wide(ra[1, k])).astype(jnp.bfloat16)
        send(None, sa.at[1, k], ry.at[1, k], (S_BY, k), (R_BY, k), dev_y)

    def stage_c(k):
        zb = order[k]
        arrive(None, rx.at[1, k], (R_CX, k))
        arrive(None, ry.at[0, k], (R_CY, k))
        arrive(None, rx.at[0, k], (R_BX, k))
        arrive(None, ry.at[1, k], (R_BY, k))
        sums = [wide(g[gblk(half, xy, zb)]) + wide(rx[half, k]) + wide(ry[half, k]) for half in range(2)]
        if k == rows - 1:
            return sums
        pz[k, 0] = sums[0].astype(jnp.bfloat16)
        pz[k, 1] = sums[1].astype(jnp.bfloat16)
        send(None, pz.at[k], rz.at[k], (S_P, k), (R_P, k), (zb, col))
        return None

    for k in range(rows):
        gradients(order[k])
        stage_a(k)
        if k >= 1:
            stage_b(k - 1)
    sums = None
    for k in range(rows):
        if k == rows - 2:
            stage_b(rows - 1)
        sums = stage_c(k)
    for k in range(rows - 1):
        arrive(None, rz.at[k], (R_P, k))
    first, second = (
        sums[half] + sum(wide(rz[k, half]) for k in range(rows - 1)) for half in range(2)
    )
    norm1 = colf[pl.ds(pl.multiple_of(xy * hp, 16), hp), :1][:hb]
    dot_first = first[:hb, ib : ib + 1]
    out1[...] = first[:hb, :ib] / norm1 - w1f[...] * (dot_first / (norm1 * norm1 * norm1))
    mine = pl.ds(pl.multiple_of(z * ip, 128), ip)
    norm2 = jnp.sqrt(1.0 + s2[0, :1, mine] + s2[1, :1, mine])[:, :ib]
    dot_second = second[hb : hb + 1, :ib]
    out2[...] = second[:hb, :ib] / norm2 - w2f[...] * (dot_second / (norm2 * norm2 * norm2))
    for cond, spec in pending:
        when(cond, lambda spec=spec: remote(*spec).wait_send())


def local_step(clean, noise, bucket, mod_table, w_first, w_second):
    rows = lax.axis_size("row")
    cols = lax.axis_size("col")
    z, col = lax.axis_index("row"), lax.axis_index("col")
    samples = bucket.shape[0]
    own_rows = clean.shape[1]
    ib, hb = clean.shape[0], w_first.shape[2]
    sub = own_rows // rows
    if sub != PIX:
        return local(clean, noise, bucket, mod_table, w_first, w_second)
    chips = cols // CORES
    hp, ip = round_up(hb + 1, 16), round_up(ib + 1, 128)
    bf16 = jnp.bfloat16
    w1f, w2f = w_first[0].T, w_second[0]
    wown = jnp.stack([w1f, w2f]).astype(bf16)
    wown = jnp.pad(wown, ((0, 0), (0, hp - hb), (0, ip - ib)))
    sample = lax.dynamic_slice_in_dim(bucket, col * rows, rows)
    levels = jnp.repeat(noise_levels(sample), PIX)[None, :]
    root = jnp.sqrt(levels * levels + 0.25)
    sto = jnp.stack([
        ((clean + levels * noise) / root).astype(bf16),
        (clean * (2.0 * levels / root) - noise * (0.5 / root)).astype(bf16),
    ])
    chip = col // CORES
    picked = jnp.stack([lax.dynamic_index_in_dim(bucket, (chip * CORES + j) * rows + z, keepdims=False) for j in range(CORES)])
    table = mod_table[0].reshape(mod_table.shape[1], chips, CORES, hb)
    mine = lax.dynamic_index_in_dim(table, lax.rem(col, CORES), axis=2, keepdims=False)
    gsel = 1.0 + jnp.take(mine, picked, axis=0)
    gsel = jnp.pad(gsel, ((0, 0), (0, 0), (0, hp - hb))).reshape(CORES, chips * hp, 1)
    hh, ii = chips * hp, rows * ip
    f32 = jnp.float32
    vmem = pl.BlockSpec(memory_space=pltpu.VMEM)
    out1, out2 = pl.pallas_call(
        lambda *refs: step_kernel(hb, ib, samples, *refs),
        out_shape=(jax.ShapeDtypeStruct((hb, ib), f32), jax.ShapeDtypeStruct((hb, ib), f32)),
        in_specs=[vmem] * 5,
        out_specs=(vmem, vmem),
        scratch_shapes=[
            pltpu.VMEM((2, hh, ii), bf16),
            pltpu.VMEM((2, ii, sub), bf16),
            pltpu.VMEM((ii, sub), bf16),
            pltpu.VMEM((2, hh, sub), f32),
            pltpu.VMEM((2, hh, sub), bf16),
            pltpu.VMEM((ii, sub), f32),
            pltpu.VMEM((ii, sub), f32),
            pltpu.VMEM((ii, sub), f32),
            pltpu.VMEM((2, ii, sub), bf16),
            pltpu.VMEM((2, ii, sub), bf16),
            pltpu.VMEM((2, hh, sub), bf16),
            pltpu.VMEM((2, 8, ii), f32),
            pltpu.VMEM((2, 8, ii), f32),
            pltpu.VMEM((2, hh, ii), bf16),
            pltpu.VMEM((2, rows, hp, ip), bf16),
            pltpu.VMEM((2, rows, hp, ip), bf16),
            pltpu.VMEM((2, rows, hp, ip), bf16),
            pltpu.VMEM((2, rows, hp, ip), bf16),
            pltpu.VMEM((rows, 2, hp, ip), bf16),
            pltpu.VMEM((rows, 2, hp, ip), bf16),
            pltpu.VMEM((hh, 128), f32),
            pltpu.SemaphoreType.DMA((32, max(rows, 11))),
        ],
        compiler_params=pltpu.CompilerParams(
            collective_id=0, has_side_effects=True, vmem_limit_bytes=60 * 1024 * 1024
        ),
    )(wown, sto, gsel, w1f, w2f)
    return (out1.T[None], out2[None])


def solution(mesh):
    placed = (
        P("row", "col"),
        P("row", "col"),
        P(),
        P(),
        P(None, "row", "col"),
        P(None, "col", "row"),
    )
    return jax.shard_map(
        local_step if mesh.shape["col"] == CORES * SIDE * SIDE else local,
        mesh=mesh,
        in_specs=placed,
        out_specs=(P(None, "row", "col"), P(None, "col", "row")),
        check_vma=False,
    )
```
